32 devices in a mesh: role: 2 (over x), ctx: 4 (over z), head: 4 (over y, core).
Axes of the slice: x: 2, y: 2, z: 4, core: 2. Of those that a mesh axis runs over, the one named last changes fastest.
Arguments:
- tokens: bfloat16 [2, 256, 7168], P('role', 'ctx', 'head'), may hold values from -6 to 6
- latent_cache: bfloat16 [192, 576], P('ctx'), may hold values from -400 to 400
- offset: int32 [1], replicated, may hold values from 49 to 192
- bounds: int32 [256], P('ctx'), may hold values from 1 to 448
- query_down: bfloat16 [7168, 1536], P('head'), may hold values from -0.0625 to 0.0625
- latent_down_weight: bfloat16 [7168, 576], P('head'), may hold values from -0.0625 to 0.0625
- query_gain: float32 [1536], replicated, may hold values from 0.25 to 1.75
- latent_norm_gain: float32 [512], replicated, may hold values from 0.25 to 1.75
- query_up: bfloat16 [1536, 24576], P(None, 'head'), may hold values from -0.15625 to 0.15625
- key_up_transposed: bfloat16 [128, 128, 512], P('head'), may hold values from -0.5 to 0.5
- value_up_weight: bfloat16 [128, 512, 128], P('head'), may hold values from -0.25 to 0.25
Outputs:
- attended: bfloat16 [2, 256, 16384], P('role', 'ctx', 'head')
The draws below stay inside these ranges and needn't reach their ends.
Inputs may be any that keep to these rules, and one draw needn't show every extreme that they name: `bounds`: A continuation row at position p sees keys at positions below p and itself. Cache slots from offset on are unused; the block's tokens sit at positions offset to offset + 255.
All inputs are finite; a program needn't handle non-finite values.
Results may differ from the reference program's by a relative error of at most 0.02.
Values may be sent and summed in bfloat16 or wider, within the bound.
No kernel may reach another device: no remote copies, remote signals or barrier semaphores. Data moves between devices by JAX's collectives and lax.ppermute only.
A program may use at most 128 MiB of HBM per device.

```python
import jax
import jax.numpy as jnp
from jax import lax

MODEL_WIDTH = 7168
QRANK = 1536
LATENT_WIDTH = 512
ROTARY_DIM = 64
PLAIN_QUERY_DIM = 128
VALUE_HEAD_SIZE = 128
ATTENTION_HEADS = 128
ROWS = 256
CACHE_SLOTS = 192


def draw_latent_cache(key, part):
    drawn_key_part, rotary_key = jax.random.split(jax.random.fold_in(key, 11), 2)
    value_rows = jnp.clip(jax.random.normal(drawn_key_part, (CACHE_SLOTS, LATENT_WIDTH + ROTARY_DIM), jnp.float32), -4.0, 4.0)
    strengths = (20.0, 45.0, 100.0)
    inserted_cache = (2, CACHE_SLOTS // 8, CACHE_SLOTS // 4)
    for element_count in range(3):
        rotation_sign = jnp.clip(jax.random.normal(jax.random.fold_in(rotary_key, element_count), (ROTARY_DIM,), jnp.float32), -3.0, 3.0)
        rotation_sign = rotation_sign * strengths[element_count]
        for second_half in range(2):
            value_rows = value_rows.at[inserted_cache[element_count] + second_half, LATENT_WIDTH:].set(rotation_sign)
    return value_rows.astype(jnp.bfloat16)


def plant(array, rng, least, high):
    place = [jax.random.randint(jax.random.fold_in(rng, axis), (), 0, length) for axis, length in enumerate(array.shape)]
    widest = array.shape.index(max(array.shape))
    next_to = place[:widest] + [(place[widest] + 1) % array.shape[widest]] + place[widest + 1:]
    return array.at[tuple(place)].set(least).at[tuple(next_to)].set(high)


def level_of(key, dims, cuts, smallest, largest):
    factor_of = 1.0
    for axis_at, blocks in cuts:
        heights = jax.random.uniform(jax.random.fold_in(jax.random.fold_in(key, 6), axis_at), (blocks,), jnp.float32, smallest / len(cuts), largest / len(cuts))
        factor_of = factor_of * jnp.repeat(jnp.exp(heights), dims[axis_at] // blocks).reshape((-1,) + (1,) * (len(dims) - 1 - axis_at))
    return factor_of


def scatter_about(stream_key, dims, scale, limit, pieces=(), kind=jnp.bfloat16):
    result = jax.random.normal(stream_key, dims, jnp.float32) * scale
    if len(pieces) > 0:
        result = level_of(stream_key, dims, pieces, -0.22, 0.18) * result
    return jnp.clip(result, min=-limit, max=limit).astype(kind)


def setup_inputs(seed: int = 0) -> dict:
    seeds = jax.random.split(jax.random.key(seed), 12)
    return {
        "tokens": scatter_about(seeds[0], (2, ROWS, MODEL_WIDTH), 1.0, 6.0, ((0, 2), (1, 4), (2, 4))),
        "latent_cache": draw_latent_cache(jax.random.fold_in(seeds[11], 71), 0),
        "offset": jax.random.randint(seeds[2], (1,), CACHE_SLOTS // 4 + 1, CACHE_SLOTS + 1).astype(jnp.int32),
        "bounds": plant(jax.random.randint(seeds[3], (ROWS,), 1, CACHE_SLOTS + ROWS + 1), jax.random.fold_in(seeds[3], 1), 1, CACHE_SLOTS + ROWS).astype(jnp.int32),
        "query_down": scatter_about(seeds[4], (MODEL_WIDTH, QRANK), MODEL_WIDTH ** -0.5, 0.0625, ((0, 4),)),
        "latent_down_weight": scatter_about(seeds[5], (MODEL_WIDTH, LATENT_WIDTH + ROTARY_DIM), MODEL_WIDTH ** -0.5, 0.0625, ((0, 4),)),
        "query_gain": jnp.clip(1.0 + 0.15 * jax.random.normal(seeds[6], (QRANK,), jnp.float32), 0.25, 1.75),
        "latent_norm_gain": jnp.clip(1.0 + 0.15 * jax.random.normal(seeds[7], (LATENT_WIDTH,), jnp.float32), 0.25, 1.75),
        "query_up": scatter_about(seeds[8], (QRANK, ATTENTION_HEADS * (PLAIN_QUERY_DIM + ROTARY_DIM)), QRANK ** -0.5, 0.15625, ((1, 4),)),
        "key_up_transposed": scatter_about(seeds[9], (ATTENTION_HEADS, PLAIN_QUERY_DIM, LATENT_WIDTH), PLAIN_QUERY_DIM ** -0.5, 0.5, ((0, 4),)),
        "value_up_weight": scatter_about(seeds[10], (ATTENTION_HEADS, LATENT_WIDTH, VALUE_HEAD_SIZE), LATENT_WIDTH ** -0.5, 0.25, ((0, 4),)),
    }


EPS = 1e-06

def root_mean_norm(value_rows, gain):
    return value_rows * lax.rsqrt(lax.optimization_barrier(jnp.mean(value_rows * value_rows, axis=-1, keepdims=True)) + EPS) * gain.astype(jnp.float32)

def apply_rotary(value_rows, token_positions):
    half = value_rows.shape[-1] // 2
    freqs = 10000.0 ** (-jnp.arange(half, dtype=jnp.float32) / half)
    angles = token_positions.astype(jnp.float32)[:, None] * freqs[None, :]
    if value_rows.ndim == 3:
        angles = angles[:, None, :]
    first = value_rows[..., :half]
    second_half = value_rows[..., half:]
    cosine = jnp.cos(angles)
    sine = jnp.sin(angles)
    return jnp.concatenate([first * cosine - second_half * sine, first * sine + second_half * cosine], axis=-1)

def project(inputs, token_positions, query_down, latent_down_weight, query_gain, latent_norm_gain, query_up, key_up_transposed):
    query_lat = jnp.dot(inputs, query_down, preferred_element_type=jnp.float32)
    key_value_latent = jnp.dot(inputs, latent_down_weight, preferred_element_type=jnp.float32)
    query_norm = root_mean_norm(query_lat, query_gain).astype(jnp.bfloat16)
    latent_vector = root_mean_norm(key_value_latent[:, :LATENT_WIDTH], latent_norm_gain)
    rotary_key_part = apply_rotary(key_value_latent[:, LATENT_WIDTH:], token_positions)
    self_key_row = jnp.concatenate([latent_vector, rotary_key_part], axis=-1).astype(jnp.bfloat16)
    queries = jnp.dot(query_norm, query_up, preferred_element_type=jnp.float32)
    queries = queries.reshape(queries.shape[0], ATTENTION_HEADS, PLAIN_QUERY_DIM + ROTARY_DIM)
    query_nope = queries[..., :PLAIN_QUERY_DIM].astype(jnp.bfloat16)
    query_rot = apply_rotary(queries[..., PLAIN_QUERY_DIM:], token_positions).astype(jnp.bfloat16)
    absorbed = jnp.einsum('rhn,hnc->rhc', query_nope.astype(jnp.float32), key_up_transposed.astype(jnp.float32)).astype(jnp.bfloat16)
    return (jnp.concatenate([absorbed, query_rot], axis=-1), self_key_row)

def attend(queries, self_key_row, limits, every_key_row, key_pos, key_valid, value_up_weight):
    softmax_scale = (PLAIN_QUERY_DIM + ROTARY_DIM) ** (-0.5)

    def one_head(operands):
        head_query, head_value = operands
        scores = jnp.dot(head_query, every_key_row.T, preferred_element_type=jnp.float32) * softmax_scale
        key_mask = key_valid[None, :] & (key_pos[None, :] < limits[:, None])
        self_score = lax.optimization_barrier(jnp.sum(head_query.astype(jnp.float32) * self_key_row.astype(jnp.float32), axis=-1)) * softmax_scale
        row_max = jnp.maximum(lax.optimization_barrier(jnp.max(jnp.where(key_mask, scores, -jnp.inf), axis=-1)), self_score)
        attention_weights = jnp.where(key_mask, jnp.exp(scores - row_max[:, None]), 0.0)
        self_attend_weight = jnp.exp(self_score - row_max)
        denom = lax.optimization_barrier(jnp.sum(attention_weights, axis=-1)) + self_attend_weight
        numerator_sum = jnp.dot(attention_weights.astype(jnp.bfloat16), every_key_row[:, :LATENT_WIDTH], preferred_element_type=jnp.float32)
        numerator_sum = numerator_sum + self_attend_weight.astype(jnp.bfloat16).astype(jnp.float32)[:, None] * self_key_row[:, :LATENT_WIDTH].astype(jnp.float32)
        out_latent = (numerator_sum / denom[:, None]).astype(jnp.bfloat16)
        return jnp.dot(out_latent, head_value, preferred_element_type=jnp.float32).astype(jnp.bfloat16)
    per_head = lax.map(one_head, (jnp.transpose(queries, (1, 0, 2)), value_up_weight))
    return jnp.transpose(per_head, (1, 0, 2)).reshape(queries.shape[0], ATTENTION_HEADS * VALUE_HEAD_SIZE)

def reference(tokens, latent_cache, offset, bounds, query_down, latent_down_weight, query_gain, latent_norm_gain, query_up, key_up_transposed, value_up_weight):
    block_start = offset[0]
    row_index = jnp.arange(ROWS, dtype=jnp.int32)
    block_pos = block_start + row_index
    weights_all = (query_down, latent_down_weight, query_gain, latent_norm_gain, query_up, key_up_transposed)
    block_query, block_key = project(tokens[0], block_pos, *weights_all)
    cont_query, cont_key = project(tokens[1], bounds, *weights_all)
    cache_pos = jnp.arange(CACHE_SLOTS, dtype=jnp.int32)
    every_key_row = jnp.concatenate([latent_cache, block_key], axis=0)
    key_pos = jnp.concatenate([cache_pos, block_pos], axis=0)
    key_valid = jnp.concatenate([cache_pos < block_start, jnp.ones((ROWS,), dtype=bool)], axis=0)
    block_out = attend(block_query, block_key, block_pos, every_key_row, key_pos, key_valid, value_up_weight)
    cont_out = attend(cont_query, cont_key, bounds, every_key_row, key_pos, key_valid, value_up_weight)
    return jnp.stack([block_out, cont_out], axis=0)
```

```python
import functools

import jax
import jax.numpy as jnp
import numpy as np
from jax import lax
from jax.experimental import pallas as pl
from jax.experimental.pallas import tpu as pltpu
from jax.sharding import PartitionSpec as P

LATENT_WIDTH = 512
ROTARY_DIM = 64
PLAIN_QUERY_DIM = 128
VALUE_HEAD_SIZE = 128
HEAD_QUERY = PLAIN_QUERY_DIM + ROTARY_DIM
KEY_WIDTH = LATENT_WIDTH + ROTARY_DIM
EPS = 1e-06
MASKED = -1e30


VMEM = pltpu.VMEM
MB = 1 << 20


def whole(memory_space=VMEM):
    return pl.BlockSpec(memory_space=memory_space)


def chunk_of(total, most):
    return max((c for c in range(128, most + 1, 128) if total % c == 0), default=total)


def in_hbm(value):
    return pltpu.with_memory_space_constraint(value, pltpu.HBM)


def parity():
    return lax.rem(lax.axis_index("head"), 2)


def rotated(value, cosine, sine):
    half = value.shape[-1] // 2
    first, second = value[:, :half], value[:, half:]
    return jnp.concatenate(
        [first * cosine - second * sine, first * sine + second * cosine], axis=-1
    )


def down_kernel(chunk, tokens, wq, wl, keep, send, wq_v, wl_v, acc, sems):
    rows, depth = tokens.shape
    half = rows // 2
    rank = wq.shape[1]
    steps = depth // chunk
    copies = []
    for i in range(steps):
        part = pl.ds(i * chunk, chunk)
        pair = (
            pltpu.make_async_copy(wq.at[part], wq_v.at[part], sems.at[0, i]),
            pltpu.make_async_copy(wl.at[:, part], wl_v.at[:, part], sems.at[1, i]),
        )
        for copy in pair:
            copy.start()
        copies.append(pair)
    for i in range(steps):
        part = pl.ds(i * chunk, chunk)
        for copy in copies[i]:
            copy.wait()
        x = tokens[:, part]
        q = jnp.dot(x, wq_v[part, :], preferred_element_type=jnp.float32)
        kv = lax.dot_general(
            x, wl_v[:, part], (((1,), (1,)), ((), ())), preferred_element_type=jnp.float32
        )
        if i == 0:
            acc[:, :rank] = q
            acc[:, rank:] = kv
        else:
            acc[:, :rank] += q
            acc[:, rank:] += kv
    c = parity()
    keep[...] = acc[pl.ds(pl.multiple_of(c * half, half), half), :]
    send[...] = acc[pl.ds(pl.multiple_of((1 - c) * half, half), half), :].astype(send.dtype)


def down(tokens, wq, wl):
    rows, depth = tokens.shape
    rank, kvw = wq.shape[1], wl.shape[0]
    chunk = chunk_of(depth, 256)
    width = rank + kvw
    return pl.pallas_call(
        functools.partial(down_kernel, chunk),
        out_shape=(
            jax.ShapeDtypeStruct((rows // 2, width), jnp.float32),
            jax.ShapeDtypeStruct((rows // 2, width), jnp.bfloat16),
        ),
        in_specs=[whole(), whole(pltpu.HBM), whole(pltpu.HBM)],
        out_specs=(whole(), whole()),
        scratch_shapes=[
            pltpu.VMEM(wq.shape, wq.dtype),
            pltpu.VMEM(wl.shape, wl.dtype),
            pltpu.VMEM((rows, width), jnp.float32),
            pltpu.SemaphoreType.DMA((2, depth // chunk)),
        ],
        compiler_params=pltpu.CompilerParams(vmem_limit_bytes=14 * MB),
        cost_estimate=pl.CostEstimate(
            flops=2 * rows * depth * width, bytes_accessed=2 * depth * width, transcendentals=0
        ),
        name="down",
    )(tokens, in_hbm(wq), in_hbm(wl))


def norm_kernel(
    peers, rank, mine, *refs
):
    own_peers, block_peers = refs[:peers], refs[peers : 2 * peers + 1]
    q_gain, kv_gain, cos_own, sin_own, cos_blk, sin_blk, latents, keys = refs[2 * peers + 1 :]
    total = mine[...]
    for ref in own_peers:
        total = total + ref[...].astype(jnp.float32)
    block = block_peers[0][...].astype(jnp.float32)
    for ref in block_peers[1:]:
        block = block + ref[...].astype(jnp.float32)
    q, kv = total[:, :rank], total[:, rank:]
    block = jnp.where(lax.axis_index("role") == 0, kv, block)

    def normed(value, gain):
        mean = jnp.mean(value * value, axis=-1, keepdims=True)
        return value * lax.rsqrt(mean + EPS) * gain[...]

    def key_of(value, cosine, sine):
        return (
            normed(value[:, :LATENT_WIDTH], kv_gain).astype(jnp.bfloat16),
            rotated(value[:, LATENT_WIDTH:], cosine[...], sine[...]).astype(jnp.bfloat16),
        )

    latents[:, :rank] = normed(q, q_gain).astype(jnp.bfloat16)
    plain, turned = key_of(kv, cos_own, sin_own)
    latents[:, rank : rank + LATENT_WIDTH] = plain
    latents[:, rank + LATENT_WIDTH :] = turned
    plain, turned = key_of(block, cos_blk, sin_blk)
    keys[:, :LATENT_WIDTH] = plain
    keys[:, LATENT_WIDTH:] = turned


def norm(mine, own_peers, block_peers, q_gain, kv_gain, tables, rank):
    half, width = mine.shape
    args = (mine, *own_peers, *block_peers, q_gain[None], kv_gain[None], *tables)
    return pl.pallas_call(
        functools.partial(norm_kernel, len(own_peers), rank),
        out_shape=(
            jax.ShapeDtypeStruct((half, width), jnp.bfloat16),
            jax.ShapeDtypeStruct((half, width - rank), jnp.bfloat16),
        ),
        in_specs=[whole()] * len(args),
        out_specs=(whole(), whole()),
        compiler_params=pltpu.CompilerParams(vmem_limit_bytes=8 * MB),
        cost_estimate=pl.CostEstimate(
            flops=20 * half * width, bytes_accessed=8 * half * width, transcendentals=0
        ),
        name="norm",
    )(*args)


def queries_kernel(own, other, cosine, sine, w_up, w_key, out, x, up, key, sems):
    half = own.shape[0]
    groups, rank, width = up.shape
    group = width // HEAD_QUERY

    def fetch(g):
        return (
            pltpu.make_async_copy(
                w_up.at[:, pl.ds(g * width, width)], up.at[g], sems.at[0, g]
            ),
            pltpu.make_async_copy(
                w_key.at[pl.ds(g * group, group)], key.at[pl.ds(g * group, group)], sems.at[1, g]
            ),
        )

    for g in range(groups):
        for copy in fetch(g):
            copy.start()
    c = parity()
    x[pl.ds(pl.multiple_of(c * half, half), half), :] = own[:, :rank]
    x[pl.ds(pl.multiple_of((1 - c) * half, half), half), :] = other[:, :rank]

    def step(g, carry):
        for copy in fetch(g):
            copy.wait()
        q = jnp.dot(x[...], up[g], preferred_element_type=jnp.float32)
        for h in range(group):
            start = h * HEAD_QUERY
            at = g * group + h
            plain = q[:, start : start + PLAIN_QUERY_DIM].astype(jnp.bfloat16)
            turned = rotated(
                q[:, start + PLAIN_QUERY_DIM : start + HEAD_QUERY], cosine[...], sine[...]
            )
            out[at, :, :LATENT_WIDTH] = jnp.dot(
                plain, key[at], preferred_element_type=jnp.float32
            ).astype(jnp.bfloat16)
            out[at, :, LATENT_WIDTH:] = turned.astype(jnp.bfloat16)
        return carry

    lax.fori_loop(0, groups, step, 0)


def queries(own, other, cosine, sine, w_up, w_key):
    rows = 2 * own.shape[0]
    rank = w_up.shape[0]
    heads = w_key.shape[0]
    group = 4
    groups = heads // group
    return pl.pallas_call(
        queries_kernel,
        out_shape=jax.ShapeDtypeStruct((heads, rows, KEY_WIDTH), jnp.bfloat16),
        in_specs=[whole()] * 4 + [whole(pltpu.HBM)] * 2,
        out_specs=whole(),
        scratch_shapes=[
            pltpu.VMEM((rows, rank), jnp.bfloat16),
            pltpu.VMEM((groups, rank, group * HEAD_QUERY), jnp.bfloat16),
            pltpu.VMEM(w_key.shape, jnp.bfloat16),
            pltpu.SemaphoreType.DMA((2, groups)),
        ],
        compiler_params=pltpu.CompilerParams(vmem_limit_bytes=32 * MB),
        cost_estimate=pl.CostEstimate(
            flops=2 * rows * heads * (rank * HEAD_QUERY + PLAIN_QUERY_DIM * LATENT_WIDTH),
            bytes_accessed=2 * heads * (rank * HEAD_QUERY + PLAIN_QUERY_DIM * LATENT_WIDTH),
            transcendentals=0,
        ),
        name="queries",
    )(own, other, cosine, sine, in_hbm(w_up), in_hbm(w_key))


def attend_kernel(pieces, scale, group, q, bias, own, other, *refs):
    parts = refs[:pieces]
    w_value, out, keys, value, sem = refs[pieces:]
    half = own.shape[0]
    copy = pltpu.make_async_copy(w_value, value, sem)
    copy.start()
    rank = own.shape[1] - KEY_WIDTH
    c = parity()
    keys[pl.ds(pl.multiple_of(c * half, half), half), :] = own[:, rank:]
    keys[pl.ds(pl.multiple_of((1 - c) * half, half), half), :] = other[:, rank:]
    at = 2 * half
    for ref in parts:
        size = ref.shape[0]
        keys[at : at + size, :] = ref[...]
        at += size
    heads, rows, width = q.shape
    count = keys.shape[0]
    copy.wait()

    for g in range(heads // group):
        k = keys[...]
        s = lax.dot_general(
            q[g * group : (g + 1) * group].reshape(group * rows, width),
            k,
            (((1,), (1,)), ((), ())),
            preferred_element_type=jnp.float32,
        )
        s = s.reshape(group, rows, count) + bias[...][None]
        m = jnp.max(s, axis=-1, keepdims=True)
        e = jnp.exp2((s - m) * scale)
        den = jnp.sum(e, axis=-1, keepdims=True)
        o = jnp.dot(
            e.astype(jnp.bfloat16).reshape(group * rows, count),
            k[:, :LATENT_WIDTH],
            preferred_element_type=jnp.float32,
        ).reshape(group, rows, LATENT_WIDTH)
        o = (o / den).astype(jnp.bfloat16)
        for i in range(group):
            h = g * group + i
            out[:, h * VALUE_HEAD_SIZE : (h + 1) * VALUE_HEAD_SIZE] = jnp.dot(
                o[i], value[h], preferred_element_type=jnp.float32
            ).astype(out.dtype)


def attend(q, bias, own, other, parts, w_value):
    heads, rows, width = q.shape
    count = bias.shape[1]
    scale = float(HEAD_QUERY ** (-0.5) * np.log2(np.e))
    group = 8 if count <= 1024 else 2
    return pl.pallas_call(
        functools.partial(attend_kernel, len(parts), scale, group),
        out_shape=jax.ShapeDtypeStruct((rows, heads * VALUE_HEAD_SIZE), jnp.bfloat16),
        in_specs=[whole()] * (4 + len(parts)) + [whole(pltpu.HBM)],
        out_specs=whole(),
        scratch_shapes=[
            pltpu.VMEM((count, width), jnp.bfloat16),
            pltpu.VMEM(w_value.shape, jnp.bfloat16),
            pltpu.SemaphoreType.DMA,
        ],
        compiler_params=pltpu.CompilerParams(vmem_limit_bytes=40 * MB),
        cost_estimate=pl.CostEstimate(
            flops=2 * rows * heads * (count * (width + LATENT_WIDTH) + LATENT_WIDTH * VALUE_HEAD_SIZE),
            bytes_accessed=2 * heads * (rows * width + LATENT_WIDTH * VALUE_HEAD_SIZE),
            transcendentals=rows * heads * count,
        ),
        name="attend",
    )(q, bias, own, other, *parts, in_hbm(w_value))


def angle_tables(positions):
    half = ROTARY_DIM // 2
    freqs = jnp.asarray(10000.0 ** (-np.arange(half) / half), jnp.float32)
    angles = positions.astype(jnp.float32)[:, None] * freqs[None, :]
    return jnp.cos(angles), jnp.sin(angles)


def local(
    tokens,
    latent_cache,
    offset,
    bounds,
    query_down,
    latent_down_weight,
    query_gain,
    latent_norm_gain,
    query_up,
    key_up_transposed,
    value_up_weight,
):
    rows = tokens.shape[1]
    half = rows // 2
    cache_rows = latent_cache.shape[0]
    rank = query_down.shape[1]
    heads = lax.axis_size("head")
    ctxs = lax.axis_size("ctx")
    role, ctx, head = (lax.axis_index(a) for a in ("role", "ctx", "head"))
    mate = [(i, i ^ 1) for i in range(heads)]
    stride = heads // 2

    block_start = offset[0]
    row = jnp.arange(rows, dtype=jnp.int32)
    block_pos = block_start + ctx * rows + row
    positions = jnp.where(role == 0, block_pos, bounds)
    mine_at = lax.rem(head, 2) * half
    cos_all, sin_all = angle_tables(positions)
    half_tables = [
        lax.dynamic_slice_in_dim(t, mine_at, half)
        for t in (cos_all, sin_all, *angle_tables(block_pos))
    ]

    at = jnp.arange(ctxs * (rows + cache_rows), dtype=jnp.int32)
    piece = at // half
    source = lax.rem(ctx + ctxs - lax.rem(piece, ctxs), ctxs)
    part = lax.rem(head + piece // ctxs, 2)
    fresh = block_start + source * rows + part * half + lax.rem(at, half)
    back = at - ctxs * rows
    source = lax.rem(ctx + ctxs - back // cache_rows, ctxs)
    cached = source * cache_rows + lax.rem(back, cache_rows)
    is_cached = back >= 0
    key_pos = jnp.where(is_cached, cached, fresh)
    key_ok = jnp.where(is_cached, cached < block_start, True)
    seen = key_ok[None, :] & (key_pos[None, :] < positions[:, None])
    itself = row[:, None] == row[None, :]
    bias = jnp.where(jnp.concatenate([itself, seen], axis=1), 0.0, MASKED).astype(jnp.float32)

    kept, sent = down(tokens[0], query_down, latent_down_weight.T)
    cache, sent = lax.optimization_barrier((latent_cache, sent))

    def shifted(value):
        return [
            lax.ppermute(value, "ctx", [(i, (i + step) % ctxs) for i in range(ctxs)])
            for step in range(1, ctxs)
        ]

    mine = kept + lax.ppermute(sent, "head", mate).astype(jnp.float32)
    wire = mine.astype(jnp.bfloat16)
    wire_kv = wire[:, rank:]
    own_peers = []
    block_peers = [lax.ppermute(wire_kv, "role", [(0, 1)])]
    for k in range(1, stride):
        turn = [(i, (i + 2 * k) % heads) for i in range(heads)]
        own_peers.append(lax.ppermute(wire, "head", turn))
        block_peers.append(
            lax.ppermute(wire_kv, ("role", "head"), [(i, heads + j) for i, j in turn])
        )
    caches = [latent_cache] + shifted(cache)
    latents, keys = norm(
        mine, own_peers, block_peers, query_gain, latent_norm_gain, half_tables, rank
    )
    other = lax.ppermute(latents, "head", mate)
    near = [keys] + shifted(keys)
    far = [lax.ppermute(keys, "head", mate)]
    q = queries(latents, other, cos_all, sin_all, query_up, key_up_transposed)
    q, *late = lax.optimization_barrier((q, *near[1:]))
    far += [lax.ppermute(p, "head", mate) for p in late]
    result = attend(q, bias, latents, other, near + far + caches, value_up_weight)
    return result[None]


def solution(mesh):
    return jax.shard_map(
        local,
        mesh=mesh,
        in_specs=(
            P("role", "ctx", "head"),
            P("ctx", None),
            P(),
            P("ctx"),
            P("head", None),
            P("head", None),
            P(),
            P(),
            P(None, "head"),
            P("head", None, None),
            P("head", None, None),
        ),
        out_specs=P("role", "ctx", "head"),
        check_vma=False,
    )
```

```python
import functools

import jax
import jax.numpy as jnp
import numpy as np
from jax import lax
from jax.experimental import pallas as pl
from jax.experimental.pallas import tpu as pltpu
from jax.sharding import PartitionSpec as P

LATENT_WIDTH = 512
ROTARY_DIM = 64
PLAIN_QUERY_DIM = 128
VALUE_HEAD_SIZE = 128
HEAD_QUERY = PLAIN_QUERY_DIM + ROTARY_DIM
KEY_WIDTH = LATENT_WIDTH + ROTARY_DIM
EPS = 1e-06
MASKED = -1e30


VMEM = pltpu.VMEM
MB = 1 << 20


def whole(memory_space=VMEM):
    return pl.BlockSpec(memory_space=memory_space)


def chunk_of(total, most):
    return max((c for c in range(128, most + 1, 128) if total % c == 0), default=total)


def cache_share(rows):
    return -(-rows // 32) * 16


def in_hbm(value):
    return pltpu.with_memory_space_constraint(value, pltpu.HBM)


def parity():
    return lax.rem(lax.axis_index("head"), 2)


def rotated(value, cosine, sine):
    half = value.shape[-1] // 2
    first, second = value[:, :half], value[:, half:]
    return jnp.concatenate(
        [first * cosine - second * sine, first * sine + second * cosine], axis=-1
    )


def down_kernel(chunk, ahead, tokens, wq, wl, keep, send, x_v, wq_v, wl_v, acc, sems):
    rows, depth = tokens.shape
    half = rows // 2
    rank = wq.shape[1]
    steps = depth // chunk
    copies = []
    for i in range(steps):
        part = pl.ds(i * chunk, chunk)
        copies.append(
            [
                pltpu.make_async_copy(wq.at[part], wq_v.at[part], sems.at[0, i]),
                pltpu.make_async_copy(wl.at[:, part], wl_v.at[:, part], sems.at[1, i]),
            ]
        )
    copies[0].append(pltpu.make_async_copy(tokens, x_v, sems.at[2, 0]))
    for batch in copies[:ahead]:
        for copy in batch:
            copy.start()
    for i in range(steps):
        part = pl.ds(i * chunk, chunk)
        for copy in copies[i]:
            copy.wait()
        if i + ahead < steps:
            for copy in copies[i + ahead]:
                copy.start()
        x = x_v[:, part]
        q = jnp.dot(x, wq_v[part, :], preferred_element_type=jnp.float32)
        kv = lax.dot_general(
            x, wl_v[:, part], (((1,), (1,)), ((), ())), preferred_element_type=jnp.float32
        )
        if i == 0:
            acc[:, :rank] = q
            acc[:, rank:] = kv
        else:
            acc[:, :rank] += q
            acc[:, rank:] += kv
    c = parity()
    keep[...] = acc[pl.ds(pl.multiple_of(c * half, half), half), :]
    send[...] = acc[pl.ds(pl.multiple_of((1 - c) * half, half), half), :].astype(send.dtype)


def down(tokens, wq, wl):
    rows, depth = tokens.shape
    rank, kvw = wq.shape[1], wl.shape[0]
    chunk = chunk_of(depth, 256)
    width = rank + kvw
    return pl.pallas_call(
        functools.partial(down_kernel, chunk, 3),
        out_shape=(
            jax.ShapeDtypeStruct((rows // 2, width), jnp.float32),
            jax.ShapeDtypeStruct((rows // 2, width), jnp.bfloat16),
        ),
        in_specs=[whole(pltpu.HBM)] * 3,
        out_specs=(whole(), whole()),
        scratch_shapes=[
            pltpu.VMEM(tokens.shape, tokens.dtype),
            pltpu.VMEM(wq.shape, wq.dtype),
            pltpu.VMEM(wl.shape, wl.dtype),
            pltpu.VMEM((rows, width), jnp.float32),
            pltpu.SemaphoreType.DMA((3, depth // chunk)),
        ],
        compiler_params=pltpu.CompilerParams(vmem_limit_bytes=14 * MB),
        cost_estimate=pl.CostEstimate(
            flops=2 * rows * depth * width, bytes_accessed=2 * depth * width, transcendentals=0
        ),
        name="down",
    )(in_hbm(tokens), in_hbm(wq), in_hbm(wl))


def norm_kernel(
    peers, rank, mine, *refs
):
    own_peers, block_peers = refs[:peers], refs[peers : 2 * peers + 1]
    cache, q_gain, kv_gain, cos_own, sin_own, cos_blk, sin_blk, latents, keys = refs[2 * peers + 1 :]
    total = mine[...]
    for ref in own_peers:
        total = total + ref[...].astype(jnp.float32)
    block = block_peers[0][...].astype(jnp.float32)
    for ref in block_peers[1:]:
        block = block + ref[...].astype(jnp.float32)
    q, kv = total[:, :rank], total[:, rank:]
    block = jnp.where(lax.axis_index("role") == 0, kv, block)

    def normed(value, gain):
        mean = jnp.mean(value * value, axis=-1, keepdims=True)
        return value * lax.rsqrt(mean + EPS) * gain[...]

    def key_of(value, cosine, sine):
        return (
            normed(value[:, :LATENT_WIDTH], kv_gain).astype(jnp.bfloat16),
            rotated(value[:, LATENT_WIDTH:], cosine[...], sine[...]).astype(jnp.bfloat16),
        )

    latents[:, :rank] = normed(q, q_gain).astype(jnp.bfloat16)
    plain, turned = key_of(kv, cos_own, sin_own)
    latents[:, rank : rank + LATENT_WIDTH] = plain
    latents[:, rank + LATENT_WIDTH :] = turned
    plain, turned = key_of(block, cos_blk, sin_blk)
    half = mine.shape[0]
    keys[:half, :LATENT_WIDTH] = plain
    keys[:half, LATENT_WIDTH:] = turned
    share = keys.shape[0] - half
    start = parity() * (cache.shape[0] - share)
    keys[half:, :] = cache[pl.ds(pl.multiple_of(start, 16), share), :]


def norm(mine, own_peers, block_peers, cache, q_gain, kv_gain, tables, rank):
    half, width = mine.shape
    args = (mine, *own_peers, *block_peers, cache, q_gain[None], kv_gain[None], *tables)
    return pl.pallas_call(
        functools.partial(norm_kernel, len(own_peers), rank),
        out_shape=(
            jax.ShapeDtypeStruct((half, width), jnp.bfloat16),
            jax.ShapeDtypeStruct((half + cache_share(cache.shape[0]), width - rank), jnp.bfloat16),
        ),
        in_specs=[whole()] * len(args),
        out_specs=(whole(), whole()),
        compiler_params=pltpu.CompilerParams(vmem_limit_bytes=8 * MB),
        cost_estimate=pl.CostEstimate(
            flops=20 * half * width, bytes_accessed=8 * half * width, transcendentals=0
        ),
        name="norm",
    )(*args)


def queries_kernel(ahead, own, other, cosine, sine, w_up, w_key, out, x, up, key, sems):
    half = own.shape[0]
    groups, rank, width = up.shape
    group = width // HEAD_QUERY

    def fetch(g):
        return (
            pltpu.make_async_copy(
                w_up.at[:, pl.ds(g * width, width)], up.at[g], sems.at[0, g]
            ),
            pltpu.make_async_copy(
                w_key.at[pl.ds(g * group, group)], key.at[pl.ds(g * group, group)], sems.at[1, g]
            ),
        )

    for g in range(min(ahead, groups)):
        for copy in fetch(g):
            copy.start()
    c = parity()
    x[pl.ds(pl.multiple_of(c * half, half), half), :] = own[:, :rank]
    x[pl.ds(pl.multiple_of((1 - c) * half, half), half), :] = other[:, :rank]

    def step(g, carry):
        for copy in fetch(g):
            copy.wait()

        @pl.when(g + ahead < groups)
        def _():
            for copy in fetch(g + ahead):
                copy.start()

        q = jnp.dot(x[...], up[g], preferred_element_type=jnp.float32)
        for h in range(group):
            start = h * HEAD_QUERY
            at = g * group + h
            plain = q[:, start : start + PLAIN_QUERY_DIM].astype(jnp.bfloat16)
            turned = rotated(
                q[:, start + PLAIN_QUERY_DIM : start + HEAD_QUERY], cosine[...], sine[...]
            )
            out[at, :, :LATENT_WIDTH] = jnp.dot(
                plain, key[at], preferred_element_type=jnp.float32
            ).astype(jnp.bfloat16)
            out[at, :, LATENT_WIDTH:] = turned.astype(jnp.bfloat16)
        return carry

    lax.fori_loop(0, groups, step, 0)


def queries(own, other, cosine, sine, w_up, w_key):
    rows = 2 * own.shape[0]
    rank = w_up.shape[0]
    heads = w_key.shape[0]
    group = 4
    groups = heads // group
    return pl.pallas_call(
        functools.partial(queries_kernel, 2),
        out_shape=jax.ShapeDtypeStruct((heads, rows, KEY_WIDTH), jnp.bfloat16),
        in_specs=[whole()] * 4 + [whole(pltpu.HBM)] * 2,
        out_specs=whole(),
        scratch_shapes=[
            pltpu.VMEM((rows, rank), jnp.bfloat16),
            pltpu.VMEM((groups, rank, group * HEAD_QUERY), jnp.bfloat16),
            pltpu.VMEM(w_key.shape, jnp.bfloat16),
            pltpu.SemaphoreType.DMA((2, groups)),
        ],
        compiler_params=pltpu.CompilerParams(vmem_limit_bytes=32 * MB),
        cost_estimate=pl.CostEstimate(
            flops=2 * rows * heads * (rank * HEAD_QUERY + PLAIN_QUERY_DIM * LATENT_WIDTH),
            bytes_accessed=2 * heads * (rank * HEAD_QUERY + PLAIN_QUERY_DIM * LATENT_WIDTH),
            transcendentals=0,
        ),
        name="queries",
    )(own, other, cosine, sine, in_hbm(w_up), in_hbm(w_key))


def attend_kernel(pieces, scale, group, q, bias, own, other, *refs):
    parts = refs[:pieces]
    w_value, out, keys, value, sem = refs[pieces:]
    half = own.shape[0]
    copy = pltpu.make_async_copy(w_value, value, sem)
    copy.start()
    rank = own.shape[1] - KEY_WIDTH
    c = parity()
    keys[pl.ds(pl.multiple_of(c * half, half), half), :] = own[:, rank:]
    keys[pl.ds(pl.multiple_of((1 - c) * half, half), half), :] = other[:, rank:]
    share = parts[0].shape[0] - half
    near = pieces // 2
    cached = (2 + pieces) * half
    room = (keys.shape[0] - cached) // near
    for i, ref in enumerate(parts):
        at = (2 + i) * half
        keys[at : at + half, :] = ref[:half, :]
        shift = (c if i < near else 1 - c) * (room - share)
        at = cached + (i % near) * room
        keys[pl.ds(pl.multiple_of(at + shift, 16), share), :] = ref[half:, :]
    heads, rows, width = q.shape
    count = keys.shape[0]
    copy.wait()

    for g in range(heads // group):
        k = keys[...]
        s = lax.dot_general(
            q[g * group : (g + 1) * group].reshape(group * rows, width),
            k,
            (((1,), (1,)), ((), ())),
            preferred_element_type=jnp.float32,
        )
        s = s.reshape(group, rows, count) + bias[...][None]
        m = jnp.max(s, axis=-1, keepdims=True)
        e = jnp.exp2((s - m) * scale)
        den = jnp.sum(e, axis=-1, keepdims=True)
        o = jnp.dot(
            e.astype(jnp.bfloat16).reshape(group * rows, count),
            k[:, :LATENT_WIDTH],
            preferred_element_type=jnp.float32,
        ).reshape(group, rows, LATENT_WIDTH)
        o = (o / den).astype(jnp.bfloat16)
        for i in range(group):
            h = g * group + i
            out[:, h * VALUE_HEAD_SIZE : (h + 1) * VALUE_HEAD_SIZE] = jnp.dot(
                o[i], value[h], preferred_element_type=jnp.float32
            ).astype(out.dtype)


def attend(q, bias, own, other, parts, w_value):
    heads, rows, width = q.shape
    count = bias.shape[1]
    scale = float(HEAD_QUERY ** (-0.5) * np.log2(np.e))
    group = 8 if count <= 1024 else 2
    return pl.pallas_call(
        functools.partial(attend_kernel, len(parts), scale, group),
        out_shape=jax.ShapeDtypeStruct((rows, heads * VALUE_HEAD_SIZE), jnp.bfloat16),
        in_specs=[whole()] * (4 + len(parts)) + [whole(pltpu.HBM)],
        out_specs=whole(),
        scratch_shapes=[
            pltpu.VMEM((count, width), jnp.bfloat16),
            pltpu.VMEM(w_value.shape, jnp.bfloat16),
            pltpu.SemaphoreType.DMA,
        ],
        compiler_params=pltpu.CompilerParams(vmem_limit_bytes=40 * MB),
        cost_estimate=pl.CostEstimate(
            flops=2 * rows * heads * (count * (width + LATENT_WIDTH) + LATENT_WIDTH * VALUE_HEAD_SIZE),
            bytes_accessed=2 * heads * (rows * width + LATENT_WIDTH * VALUE_HEAD_SIZE),
            transcendentals=rows * heads * count,
        ),
        name="attend",
    )(q, bias, own, other, *parts, in_hbm(w_value))


def angle_tables(positions):
    half = ROTARY_DIM // 2
    freqs = jnp.asarray(10000.0 ** (-np.arange(half) / half), jnp.float32)
    angles = positions.astype(jnp.float32)[:, None] * freqs[None, :]
    return jnp.cos(angles), jnp.sin(angles)


def local(
    tokens,
    latent_cache,
    offset,
    bounds,
    query_down,
    latent_down_weight,
    query_gain,
    latent_norm_gain,
    query_up,
    key_up_transposed,
    value_up_weight,
):
    rows = tokens.shape[1]
    half = rows // 2
    cache_rows = latent_cache.shape[0]
    rank = query_down.shape[1]
    heads = lax.axis_size("head")
    ctxs = lax.axis_size("ctx")
    role, ctx, head = (lax.axis_index(a) for a in ("role", "ctx", "head"))
    mate = [(i, i ^ 1) for i in range(heads)]
    stride = heads // 2

    block_start = offset[0]
    row = jnp.arange(rows, dtype=jnp.int32)
    block_pos = block_start + ctx * rows + row
    positions = jnp.where(role == 0, block_pos, bounds)
    mine_at = lax.rem(head, 2) * half
    cos_all, sin_all = angle_tables(positions)
    half_tables = [
        lax.dynamic_slice_in_dim(t, mine_at, half)
        for t in (cos_all, sin_all, *angle_tables(block_pos))
    ]

    at = jnp.arange(ctxs * (rows + cache_rows), dtype=jnp.int32)
    piece = at // half
    source = lax.rem(ctx + ctxs - lax.rem(piece, ctxs), ctxs)
    part = lax.rem(head + piece // ctxs, 2)
    fresh = block_start + source * rows + part * half + lax.rem(at, half)
    back = at - ctxs * rows
    source = lax.rem(ctx + ctxs - back // cache_rows, ctxs)
    cached = source * cache_rows + lax.rem(back, cache_rows)
    is_cached = back >= 0
    key_pos = jnp.where(is_cached, cached, fresh)
    key_ok = jnp.where(is_cached, cached < block_start, True)
    seen = key_ok[None, :] & (key_pos[None, :] < positions[:, None])
    itself = row[:, None] == row[None, :]
    bias = jnp.where(jnp.concatenate([itself, seen], axis=1), 0.0, MASKED).astype(jnp.float32)

    kept, sent = down(tokens[0], query_down, latent_down_weight.T)
    def shifted(value):
        return [
            lax.ppermute(value, "ctx", [(i, (i + step) % ctxs) for i in range(ctxs)])
            for step in range(1, ctxs)
        ]

    mine = kept + lax.ppermute(sent, "head", mate).astype(jnp.float32)
    wire = mine.astype(jnp.bfloat16)
    wire_kv = wire[:, rank:]
    own_peers = []
    block_peers = [lax.ppermute(wire_kv, "role", [(0, 1)])]
    for k in range(1, stride):
        turn = [(i, (i + 2 * k) % heads) for i in range(heads)]
        own_peers.append(lax.ppermute(wire, "head", turn))
        block_peers.append(
            lax.ppermute(wire_kv, ("role", "head"), [(i, heads + j) for i, j in turn])
        )
    latents, keys = norm(
        mine, own_peers, block_peers, latent_cache, query_gain, latent_norm_gain, half_tables, rank
    )
    other = lax.ppermute(latents, "head", mate)
    near = [keys] + shifted(keys)
    far = [lax.ppermute(keys, "head", mate)]
    q = queries(latents, other, cos_all, sin_all, query_up, key_up_transposed)
    q, *late = lax.optimization_barrier((q, *near[1:]))
    far += [lax.ppermute(p, "head", mate) for p in late]
    result = attend(q, bias, latents, other, near + far, value_up_weight)
    return result[None]


def solution(mesh):
    return jax.shard_map(
        local,
        mesh=mesh,
        in_specs=(
            P("role", "ctx", "head"),
            P("ctx", None),
            P(),
            P("ctx"),
            P("head", None),
            P("head", None),
            P(),
            P(),
            P(None, "head"),
            P("head", None, None),
            P("head", None, None),
        ),
        out_specs=P("role", "ctx", "head"),
        check_vma=False,
    )
```

```python
import functools

import jax
import jax.numpy as jnp
import numpy as np
from jax import lax
from jax.experimental import pallas as pl
from jax.experimental.pallas import tpu as pltpu
from jax.sharding import PartitionSpec as P

LATENT_WIDTH = 512
ROTARY_DIM = 64
PLAIN_QUERY_DIM = 128
VALUE_HEAD_SIZE = 128
HEAD_QUERY = PLAIN_QUERY_DIM + ROTARY_DIM
KEY_WIDTH = LATENT_WIDTH + ROTARY_DIM
EPS = 1e-06
MASKED = -1e30


VMEM = pltpu.VMEM
MB = 1 << 20


def whole(memory_space=VMEM):
    return pl.BlockSpec(memory_space=memory_space)


def chunk_of(total, most):
    return max((c for c in range(128, most + 1, 128) if total % c == 0), default=total)


def cache_share(rows):
    return -(-rows // 32) * 16


def in_hbm(value):
    return pltpu.with_memory_space_constraint(value, pltpu.HBM)


def parity():
    return lax.rem(lax.axis_index("head"), 2)


def rotated(value, cosine, sine):
    half = value.shape[-1] // 2
    first, second = value[:, :half], value[:, half:]
    return jnp.concatenate(
        [first * cosine - second * sine, first * sine + second * cosine], axis=-1
    )


def down_kernel(chunk, ahead, tokens, wq, wl, keep, send, x_v, wq_v, wl_v, acc, sems):
    rows, depth = tokens.shape
    half = rows // 2
    rank = wq.shape[1]
    steps = depth // chunk
    copies = []
    for i in range(steps):
        part = pl.ds(i * chunk, chunk)
        copies.append(
            [
                pltpu.make_async_copy(wq.at[part], wq_v.at[part], sems.at[0, i]),
                pltpu.make_async_copy(wl.at[:, part], wl_v.at[:, part], sems.at[1, i]),
            ]
        )
    copies[0].append(pltpu.make_async_copy(tokens, x_v, sems.at[2, 0]))
    for batch in copies[:ahead]:
        for copy in batch:
            copy.start()
    for i in range(steps):
        part = pl.ds(i * chunk, chunk)
        for copy in copies[i]:
            copy.wait()
        if i + ahead < steps:
            for copy in copies[i + ahead]:
                copy.start()
        x = x_v[:, part]
        q = jnp.dot(x, wq_v[part, :], preferred_element_type=jnp.float32)
        kv = lax.dot_general(
            x, wl_v[:, part], (((1,), (1,)), ((), ())), preferred_element_type=jnp.float32
        )
        if i == 0:
            acc[:, :rank] = q
            acc[:, rank:] = kv
        else:
            acc[:, :rank] += q
            acc[:, rank:] += kv
    c = parity()
    keep[...] = acc[pl.ds(pl.multiple_of(c * half, half), half), :]
    send[...] = acc[pl.ds(pl.multiple_of((1 - c) * half, half), half), :].astype(send.dtype)


def down(tokens, wq, wl):
    rows, depth = tokens.shape
    rank, kvw = wq.shape[1], wl.shape[0]
    chunk = chunk_of(depth, 256)
    width = rank + kvw
    return pl.pallas_call(
        functools.partial(down_kernel, chunk, 3),
        out_shape=(
            jax.ShapeDtypeStruct((rows // 2, width), jnp.float32),
            jax.ShapeDtypeStruct((rows // 2, width), jnp.bfloat16),
        ),
        in_specs=[whole(pltpu.HBM)] * 3,
        out_specs=(whole(), whole()),
        scratch_shapes=[
            pltpu.VMEM(tokens.shape, tokens.dtype),
            pltpu.VMEM(wq.shape, wq.dtype),
            pltpu.VMEM(wl.shape, wl.dtype),
            pltpu.VMEM((rows, width), jnp.float32),
            pltpu.SemaphoreType.DMA((3, depth // chunk)),
        ],
        compiler_params=pltpu.CompilerParams(vmem_limit_bytes=14 * MB),
        cost_estimate=pl.CostEstimate(
            flops=2 * rows * depth * width, bytes_accessed=2 * depth * width, transcendentals=0
        ),
        name="down",
    )(in_hbm(tokens), in_hbm(wq), in_hbm(wl))


def fold_kernel(kept, got, mine, wire, wire_kv):
    total = kept[...] + got[...].astype(jnp.float32)
    rounded = total.astype(wire.dtype)
    mine[...] = total
    wire[...] = rounded
    wire_kv[...] = rounded[:, wire.shape[1] - wire_kv.shape[1] :]


def fold(kept, got):
    half, width = kept.shape
    return pl.pallas_call(
        fold_kernel,
        out_shape=(
            jax.ShapeDtypeStruct((half, width), jnp.float32),
            jax.ShapeDtypeStruct((half, width), jnp.bfloat16),
            jax.ShapeDtypeStruct((half, KEY_WIDTH), jnp.bfloat16),
        ),
        in_specs=[whole()] * 2,
        out_specs=[whole()] * 3,
        compiler_params=pltpu.CompilerParams(vmem_limit_bytes=4 * MB),
        cost_estimate=pl.CostEstimate(
            flops=40 * 10**9, bytes_accessed=40 * MB, transcendentals=0
        ),
        name="fold",
    )(kept, got)


def norm_kernel(
    peers, rank, mine, *refs
):
    own_peers, block_peers = refs[:peers], refs[peers : 2 * peers + 1]
    cache, q_gain, kv_gain, cos_own, sin_own, cos_blk, sin_blk, latents, keys = refs[2 * peers + 1 :]
    total = mine[...]
    for ref in own_peers:
        total = total + ref[...].astype(jnp.float32)
    block = block_peers[0][...].astype(jnp.float32)
    for ref in block_peers[1:]:
        block = block + ref[...].astype(jnp.float32)
    q, kv = total[:, :rank], total[:, rank:]
    block = jnp.where(lax.axis_index("role") == 0, kv, block)

    def normed(value, gain):
        mean = jnp.mean(value * value, axis=-1, keepdims=True)
        return value * lax.rsqrt(mean + EPS) * gain[...]

    def key_of(value, cosine, sine):
        return (
            normed(value[:, :LATENT_WIDTH], kv_gain).astype(jnp.bfloat16),
            rotated(value[:, LATENT_WIDTH:], cosine[...], sine[...]).astype(jnp.bfloat16),
        )

    latents[:, :rank] = normed(q, q_gain).astype(jnp.bfloat16)
    plain, turned = key_of(kv, cos_own, sin_own)
    latents[:, rank : rank + LATENT_WIDTH] = plain
    latents[:, rank + LATENT_WIDTH :] = turned
    plain, turned = key_of(block, cos_blk, sin_blk)
    half = mine.shape[0]
    keys[:half, :LATENT_WIDTH] = plain
    keys[:half, LATENT_WIDTH:] = turned
    share = keys.shape[0] - half
    start = parity() * (cache.shape[0] - share)
    keys[half:, :] = cache[pl.ds(pl.multiple_of(start, 16), share), :]


def norm(mine, own_peers, block_peers, cache, q_gain, kv_gain, tables, rank):
    half, width = mine.shape
    args = (mine, *own_peers, *block_peers, cache, q_gain[None], kv_gain[None], *tables)
    return pl.pallas_call(
        functools.partial(norm_kernel, len(own_peers), rank),
        out_shape=(
            jax.ShapeDtypeStruct((half, width), jnp.bfloat16),
            jax.ShapeDtypeStruct((half + cache_share(cache.shape[0]), width - rank), jnp.bfloat16),
        ),
        in_specs=[whole()] * len(args),
        out_specs=(whole(), whole()),
        compiler_params=pltpu.CompilerParams(vmem_limit_bytes=8 * MB),
        cost_estimate=pl.CostEstimate(
            flops=20 * half * width, bytes_accessed=8 * half * width, transcendentals=0
        ),
        name="norm",
    )(*args)


def queries_kernel(own, other, cosine, sine, w_up, w_key, out, x, held):
    half = own.shape[0]
    rank = x.shape[1]
    heads = w_key.shape[0]
    width = held.shape[2]
    group = width // HEAD_QUERY
    groups = heads // group
    c = parity()
    x[pl.ds(pl.multiple_of(c * half, half), half), :] = own[:, :rank]
    x[pl.ds(pl.multiple_of((1 - c) * half, half), half), :] = other[:, :rank]

    def project(g):
        held[g % 2] = jnp.dot(
            x[...], w_up[:, g * width : (g + 1) * width], preferred_element_type=jnp.float32
        )

    project(0)
    for g in range(groups):
        if g + 1 < groups:
            project(g + 1)
        q = held.at[g % 2]
        for h in range(group):
            start = h * HEAD_QUERY
            plain = q[:, start : start + PLAIN_QUERY_DIM].astype(jnp.bfloat16)
            out[g * group + h, :, :LATENT_WIDTH] = jnp.dot(
                plain, w_key[g * group + h], preferred_element_type=jnp.float32
            ).astype(jnp.bfloat16)
        for h in range(group):
            start = h * HEAD_QUERY + PLAIN_QUERY_DIM
            turned = rotated(q[:, start : start + ROTARY_DIM], cosine[...], sine[...])
            out[g * group + h, :, LATENT_WIDTH:] = turned.astype(jnp.bfloat16)


def queries(own, other, cosine, sine, w_up, w_key):
    rows = 2 * own.shape[0]
    rank = w_up.shape[0]
    heads = w_key.shape[0]
    return pl.pallas_call(
        queries_kernel,
        out_shape=jax.ShapeDtypeStruct((heads, rows, KEY_WIDTH), jnp.bfloat16),
        in_specs=[whole()] * 6,
        out_specs=whole(),
        scratch_shapes=[
            pltpu.VMEM((rows, rank), jnp.bfloat16),
            pltpu.VMEM((2, rows, min(8, heads) * HEAD_QUERY), jnp.float32),
        ],
        compiler_params=pltpu.CompilerParams(vmem_limit_bytes=8 * MB),
        cost_estimate=pl.CostEstimate(
            flops=2 * rows * heads * (rank * HEAD_QUERY + PLAIN_QUERY_DIM * LATENT_WIDTH),
            bytes_accessed=2 * heads * (rank * HEAD_QUERY + PLAIN_QUERY_DIM * LATENT_WIDTH),
            transcendentals=0,
        ),
        name="queries",
    )(own, other, cosine, sine, w_up, w_key)


def attend_kernel(pieces, scale, group, q, bias, own, other, *refs):
    parts = refs[:pieces]
    value, out, keys = refs[pieces:]
    half = own.shape[0]
    rank = own.shape[1] - KEY_WIDTH
    c = parity()
    keys[pl.ds(pl.multiple_of(c * half, half), half), :] = own[:, rank:]
    keys[pl.ds(pl.multiple_of((1 - c) * half, half), half), :] = other[:, rank:]
    share = parts[0].shape[0] - half
    near = pieces // 2
    cached = (2 + pieces) * half
    room = (keys.shape[0] - cached) // near
    for i, ref in enumerate(parts):
        at = (2 + i) * half
        keys[at : at + half, :] = ref[:half, :]
        shift = (c if i < near else 1 - c) * (room - share)
        at = cached + (i % near) * room
        keys[pl.ds(pl.multiple_of(at + shift, 16), share), :] = ref[half:, :]
    heads, rows, width = q.shape
    count = keys.shape[0]

    for g in range(heads // group):
        k = keys[...]
        s = lax.dot_general(
            q[g * group : (g + 1) * group].reshape(group * rows, width),
            k,
            (((1,), (1,)), ((), ())),
            preferred_element_type=jnp.float32,
        )
        s = s.reshape(group, rows, count) + bias[...][None]
        m = jnp.max(s, axis=-1, keepdims=True)
        e = jnp.exp2((s - m) * scale)
        den = jnp.sum(e, axis=-1, keepdims=True)
        o = jnp.dot(
            e.astype(jnp.bfloat16).reshape(group * rows, count),
            k[:, :LATENT_WIDTH],
            preferred_element_type=jnp.float32,
        ).reshape(group, rows, LATENT_WIDTH)
        o = (o / den).astype(jnp.bfloat16)
        for i in range(group):
            h = g * group + i
            out[:, h * VALUE_HEAD_SIZE : (h + 1) * VALUE_HEAD_SIZE] = jnp.dot(
                o[i], value[h], preferred_element_type=jnp.float32
            ).astype(out.dtype)


def attend(q, bias, own, other, parts, w_value):
    heads, rows, width = q.shape
    count = bias.shape[1]
    scale = float(HEAD_QUERY ** (-0.5) * np.log2(np.e))
    group = 8 if count <= 1024 else 2
    return pl.pallas_call(
        functools.partial(attend_kernel, len(parts), scale, group),
        out_shape=jax.ShapeDtypeStruct((rows, heads * VALUE_HEAD_SIZE), jnp.bfloat16),
        in_specs=[whole()] * (5 + len(parts)),
        out_specs=whole(),
        scratch_shapes=[
            pltpu.VMEM((count, width), jnp.bfloat16),
        ],
        compiler_params=pltpu.CompilerParams(vmem_limit_bytes=24 * MB),
        cost_estimate=pl.CostEstimate(
            flops=2 * rows * heads * (count * (width + LATENT_WIDTH) + LATENT_WIDTH * VALUE_HEAD_SIZE),
            bytes_accessed=2 * heads * (rows * width + LATENT_WIDTH * VALUE_HEAD_SIZE),
            transcendentals=rows * heads * count,
        ),
        name="attend",
    )(q, bias, own, other, *parts, w_value)


def angle_tables(positions):
    half = ROTARY_DIM // 2
    freqs = jnp.asarray(10000.0 ** (-np.arange(half) / half), jnp.float32)
    angles = positions.astype(jnp.float32)[:, None] * freqs[None, :]
    return jnp.cos(angles), jnp.sin(angles)


def local(
    tokens,
    latent_cache,
    offset,
    bounds,
    query_down,
    latent_down_weight,
    query_gain,
    latent_norm_gain,
    query_up,
    key_up_transposed,
    value_up_weight,
):
    rows = tokens.shape[1]
    half = rows // 2
    cache_rows = latent_cache.shape[0]
    rank = query_down.shape[1]
    heads = lax.axis_size("head")
    ctxs = lax.axis_size("ctx")
    role, ctx, head = (lax.axis_index(a) for a in ("role", "ctx", "head"))
    mate = [(i, i ^ 1) for i in range(heads)]
    stride = heads // 2

    block_start = offset[0]
    row = jnp.arange(rows, dtype=jnp.int32)
    block_pos = block_start + ctx * rows + row
    positions = jnp.where(role == 0, block_pos, bounds)
    mine_at = lax.rem(head, 2) * half
    cos_all, sin_all = angle_tables(positions)
    half_tables = [
        lax.dynamic_slice_in_dim(t, mine_at, half)
        for t in (cos_all, sin_all, *angle_tables(block_pos))
    ]

    at = jnp.arange(ctxs * (rows + cache_rows), dtype=jnp.int32)
    piece = at // half
    source = ctx ^ lax.rem(piece, ctxs)
    part = lax.rem(head + piece // ctxs, 2)
    fresh = block_start + source * rows + part * half + lax.rem(at, half)
    back = at - ctxs * rows
    source = ctx ^ (back // cache_rows)
    cached = source * cache_rows + lax.rem(back, cache_rows)
    is_cached = back >= 0
    key_pos = jnp.where(is_cached, cached, fresh)
    key_ok = jnp.where(is_cached, cached < block_start, True)
    seen = key_ok[None, :] & (key_pos[None, :] < positions[:, None])
    itself = row[:, None] == row[None, :]
    bias = jnp.where(jnp.concatenate([itself, seen], axis=1), 0.0, MASKED).astype(jnp.float32)

    kept, sent = down(tokens[0], query_down, latent_down_weight.T)
    def shifted(value):
        return [
            lax.ppermute(value, "ctx", [(i, i ^ step) for i in range(ctxs)])
            for step in range(1, ctxs)
        ]

    mine, wire, wire_kv = fold(kept, lax.ppermute(sent, "head", mate))
    own_peers, block_peers = [], []
    for k in range(1, stride):
        turn = [(i, (i + 2 * k) % heads) for i in range(heads)]
        own_peers.append(lax.ppermute(wire, "head", turn))
        block_peers.append(
            lax.ppermute(wire_kv, ("role", "head"), [(i, heads + j) for i, j in turn])
        )
    block_peers.append(lax.ppermute(wire_kv, "role", [(0, 1)]))
    latents, keys = norm(
        mine, own_peers, block_peers, latent_cache, query_gain, latent_norm_gain, half_tables, rank
    )
    other = lax.ppermute(latents, "head", mate)
    near = [keys] + shifted(keys)
    far = [lax.ppermute(keys, "head", mate)]
    q = queries(latents, other, cos_all, sin_all, query_up, key_up_transposed)
    q, *late = lax.optimization_barrier((q, *near[1:]))
    far += [lax.ppermute(p, "head", mate) for p in late]
    result = attend(q, bias, latents, other, near + far, value_up_weight)
    return result[None]


def solution(mesh):
    return jax.shard_map(
        local,
        mesh=mesh,
        in_specs=(
            P("role", "ctx", "head"),
            P("ctx", None),
            P(),
            P("ctx"),
            P("head", None),
            P("head", None),
            P(),
            P(),
            P(None, "head"),
            P("head", None, None),
            P("head", None, None),
        ),
        out_specs=P("role", "ctx", "head"),
        check_vma=False,
    )
```
